32 devices in a mesh: seq: 8 (over y, x, core), tp: 4 (over z).
Axes of the slice: x: 2, y: 2, z: 4, core: 2. Of those that a mesh axis runs over, the one named last changes fastest.
Arguments:
- hidden_in: bfloat16 [4096, 2048], P('seq', 'tp'), may hold values from -60 to 60
- w_query: bfloat16 [2048, 2048], P(None, 'tp'), may hold values from -0.125 to 0.125
- w_key: bfloat16 [2048, 2048], P(None, 'tp'), may hold values from -0.125 to 0.125
- w_value: bfloat16 [2048, 2048], P(None, 'tp'), may hold values from -0.8984375 to 0.8984375
- w_pos: bfloat16 [2048, 2048], P(None, 'tp'), may hold values from -0.125 to 0.125
- w_out: bfloat16 [2048, 2048], P('tp'), may hold values from -0.125 to 0.125
- bias_content: float32 [16, 128], P('tp'), may hold values from -4 to 4
- bias_pos: float32 [16, 128], P('tp'), may hold values from -4 to 4
- norm_gain: float32 [2048], P('tp'), may hold values from 0.1 to 1.9
- norm_bias: float32 [2048], P('tp'), may hold values from -3 to 3
Outputs:
- hidden_out: bfloat16 [4096, 2048], P('seq', 'tp')
The draws below stay inside these ranges and needn't reach their ends.
All inputs are finite; a program needn't handle non-finite values.
Results may differ from the reference program's by a relative error of at most 0.014.
The reference program's roundings to bfloat16 on the way count: a program that leaves them out, or rounds other values in their place, can miss the bound.
Values may be sent and summed in bfloat16 or wider, within the bound.
A program may use at most 128 MiB of HBM per device.

```python
import jax
import jax.numpy as jnp
from jax import lax

D = 2048
HEADS = 16
HEAD_DIM = 128
SEG = 512
TOKENS = 4096
N_SEQ = 8
N_TP = 4


def draw_hidden_in(key, part):
    first, second, third = jax.random.split(key, 3)
    base = jax.random.normal(first, (TOKENS, D), jnp.float32)
    columns = jnp.exp(jnp.log(3.0) * jnp.arange(D).astype(jnp.float32) / D)
    columns = columns * jax.random.uniform(second, (D,), jnp.float32, minval=0.7, maxval=1.4)
    rows = jnp.exp(jax.random.uniform(third, (TOKENS, 1), jnp.float32, minval=0.0, maxval=jnp.log(2.0)))
    value = base * rows * columns[None, :]
    return jnp.clip(value, -60.0, 60.0).astype(jnp.bfloat16)


def levels(own_key, dims, pieces, least, top_value):
    def one(dim, parts):
        heights = jax.random.uniform(jax.random.fold_in(jax.random.fold_in(own_key, 6), dim), (parts,), jnp.float32, least / len(pieces), top_value / len(pieces))
        return jnp.repeat(jnp.exp(heights), dims[dim] // parts).reshape((-1,) + (1,) * (len(dims) - dim - 1))

    gain = one(*pieces[0])
    for cut in pieces[1:]:
        gain = gain * one(*cut)
    return gain


def scatter_about(own_key, extent, deviation, bound, shards=(), held_as=jnp.bfloat16):
    values = jax.random.normal(own_key, extent, jnp.float32) * deviation
    if len(shards) > 0:
        values = levels(own_key, extent, shards, -0.22, 0.18) * values
    return jnp.clip(values, min=-bound, max=bound).astype(held_as)


def setup_inputs(seed: int = 0) -> dict:
    splits = jax.random.split(jax.random.key(seed), 11)
    hidden_in = draw_hidden_in(jax.random.fold_in(splits[10], 71), 0)
    w_query = scatter_about(splits[1], (D, HEADS * HEAD_DIM), D ** -0.5, 0.125, ((1, 4),))
    w_key = scatter_about(splits[2], (D, HEADS * HEAD_DIM), D ** -0.5, 0.125, ((1, 4),))
    w_value = scatter_about(splits[3], (D, HEADS * HEAD_DIM), 0.15, 0.8984375, ((1, 4),))
    w_pos = scatter_about(splits[4], (D, HEADS * HEAD_DIM), D ** -0.5, 0.125, ((1, 4),))
    w_out = scatter_about(splits[5], (HEADS * HEAD_DIM, D), (HEADS * HEAD_DIM) ** -0.5, 0.125, ((0, 4),))
    bias_content = scatter_about(splits[6], (HEADS, HEAD_DIM), 1.0, 4.0, ((0, 4),), jnp.float32)
    bias_pos = scatter_about(splits[7], (HEADS, HEAD_DIM), 1.0, 4.0, ((0, 4),), jnp.float32)
    norm_gain = jnp.clip(1.0 + 0.18 * jax.random.normal(splits[8], (D,), jnp.float32), 0.1, 1.9)
    norm_bias = scatter_about(splits[9], (D,), 0.5, 3.0, ((0, 4),), jnp.float32)
    return dict(hidden_in=hidden_in, w_query=w_query, w_key=w_key, w_value=w_value, w_pos=w_pos, w_out=w_out, bias_content=bias_content, bias_pos=bias_pos, norm_gain=norm_gain, norm_bias=norm_bias)


def relative_table(span, width):
    half = width // 2
    freq = jnp.exp(-jnp.log(10000.0) * jnp.arange(half).astype(jnp.float32) / half)
    distance = (span - 1 - jnp.arange(span)).astype(jnp.float32)
    angle = distance[:, None] * freq[None, :]
    return jnp.concatenate([jnp.sin(angle), jnp.cos(angle)], 1).astype(jnp.bfloat16)

def shift_rows(table, seg, span):
    heads = table.shape[0]
    padded = jnp.pad(table, ((0, 0), (0, 0), (0, 1)))
    flat = padded.reshape(heads, seg * (span + 1))
    return flat[:, seg - 1:seg - 1 + seg * span].reshape(heads, seg, span)

def reference(hidden_in, w_query, w_key, w_value, w_pos, w_out, bias_content, bias_pos, norm_gain, norm_bias):
    span = 3 * SEG
    memory = 2 * SEG
    width = HEADS * HEAD_DIM
    query = jnp.dot(hidden_in, w_query, preferred_element_type=jnp.float32).astype(jnp.bfloat16)
    keys = jnp.dot(hidden_in, w_key, preferred_element_type=jnp.float32).astype(jnp.bfloat16)
    values = jnp.dot(hidden_in, w_value, preferred_element_type=jnp.float32).astype(jnp.bfloat16)
    rel = jnp.dot(relative_table(span, D), w_pos, preferred_element_type=jnp.float32).astype(jnp.bfloat16)
    rel = rel.reshape(span, HEADS, HEAD_DIM).astype(jnp.float32)
    front = jnp.zeros((memory, width), jnp.bfloat16)
    pad_keys = jnp.concatenate([front, keys], 0)
    pad_values = jnp.concatenate([front, values], 0)
    scale = 1.0 / jnp.sqrt(jnp.float32(HEAD_DIM))

    def one_segment(index):
        start = (index * SEG).astype(jnp.int32)
        q_rows = lax.dynamic_slice_in_dim(query, start, SEG, 0).astype(jnp.float32).reshape(SEG, HEADS, HEAD_DIM)
        k_rows = lax.dynamic_slice_in_dim(pad_keys, start, span, 0).astype(jnp.float32).reshape(span, HEADS, HEAD_DIM)
        v_rows = lax.dynamic_slice_in_dim(pad_values, start, span, 0).astype(jnp.float32).reshape(span, HEADS, HEAD_DIM)
        content_q = (q_rows + bias_content[None]).astype(jnp.bfloat16).astype(jnp.float32)
        pos_q = (q_rows + bias_pos[None]).astype(jnp.bfloat16).astype(jnp.float32)
        content = jnp.einsum('ihd,jhd->hij', content_q, k_rows)
        position = shift_rows(jnp.einsum('ihd,ehd->hie', pos_q, rel), SEG, span)
        score = (content + position) * scale
        row = jnp.arange(SEG)[:, None]
        col = jnp.arange(span)[None, :]
        allowed = (col <= row + memory) & (start - memory + col >= 0)
        score = jnp.where(allowed[None], score, jnp.float32(-1e+30))
        probs = jax.nn.softmax(score, axis=-1).astype(jnp.bfloat16).astype(jnp.float32)
        attended = jnp.einsum('hij,jhd->ihd', probs, v_rows)
        return attended.astype(jnp.bfloat16).reshape(SEG, width)
    attended = lax.map(one_segment, jnp.arange(N_SEQ).astype(jnp.int32)).reshape(TOKENS, width)
    group = width // N_TP
    branch = jnp.zeros((TOKENS, D), jnp.float32)
    for part in range(N_TP):
        piece = jnp.dot(attended[:, part * group:(part + 1) * group], w_out[part * group:(part + 1) * group], preferred_element_type=jnp.float32)
        branch = branch + piece.astype(jnp.bfloat16).astype(jnp.float32)
    summed = hidden_in.astype(jnp.float32) + branch
    center = lax.optimization_barrier(jnp.mean(summed, axis=1, keepdims=True))
    spread = lax.optimization_barrier(jnp.mean((summed - center) ** 2, axis=1, keepdims=True))
    normed = (summed - center) / jnp.sqrt(spread + 1e-05)
    return (normed * norm_gain[None] + norm_bias[None]).astype(jnp.bfloat16)
```

```python
import functools

import jax
import jax.numpy as jnp
import numpy as np
from jax import lax
from jax.experimental import pallas as pl
from jax.experimental.pallas import tpu as pltpu
from jax.sharding import PartitionSpec as P

F32 = jnp.float32
BF16 = jnp.bfloat16
ROWS = 128


def angle_tables(span, width):
    half = width // 2
    freq = np.exp(-np.log(10000.0) * np.arange(half) / half)
    fine = (ROWS - 1 - np.arange(ROWS))[:, None] * freq[None]
    blocks = span // ROWS
    coarse = (ROWS * (blocks - 1 - np.arange(blocks)))[:, None] * freq[None]
    pack = lambda a: np.concatenate([np.sin(a), np.cos(a)], 1).astype(np.float32)
    return pack(fine), pack(coarse)


def kernel(
    n_seq,
    n_tp,
    hidden,
    wq_hbm,
    wk_hbm,
    wv_hbm,
    wpos_hbm,
    wout_hbm,
    fine_hbm,
    coarse,
    bias_c,
    bias_p,
    gain,
    shift,
    out,
    w_all,
    w_pos,
    w_out,
    fine,
    full,
    k_t,
    val,
    rel_t,
    emb,
    cq,
    pq,
    att,
    sum_own,
    part,
    got,
    stat,
    stat_got,
    local_sem,
    ag_send,
    ag_recv,
    kv_send,
    kv_recv,
    rs_send,
    rs_recv,
    st_send,
    st_recv,
):
    seg, feat = hidden.shape
    heads, head_dim = bias_c.shape
    width = heads * head_dim
    model = n_tp * feat
    span = 3 * seg
    memory = 2 * seg
    chunks = seg // ROWS
    me = lax.axis_index("tp")
    place = lax.axis_index("seq")
    right = lax.rem(me + 1, n_tp)
    left = lax.rem(me + n_tp - 1, n_tp)
    opp = lax.rem(me + 2, n_tp)
    following = lax.rem(place + 1, n_seq)
    before = lax.rem(place + n_seq - 1, n_seq)

    loads = []
    for i, (src, dst) in enumerate(
        (
            (fine_hbm, fine),
            (wpos_hbm, w_pos),
            (wq_hbm, w_all.at[:, 0:width]),
            (wk_hbm, w_all.at[:, width : 2 * width]),
            (wv_hbm, w_all.at[:, 2 * width : 3 * width]),
            (wout_hbm, w_out),
        )
    ):
        load = pltpu.make_async_copy(src, dst, local_sem.at[i])
        load.start()
        loads.append(load)

    barrier = pltpu.get_barrier_semaphore()
    for peer in ({"tp": right}, {"tp": left}, {"tp": opp}, {"seq": following}, {"seq": before}):
        pl.semaphore_signal(barrier, inc=1, device_id=peer, device_id_type=pl.DeviceIdType.MESH)
    pl.semaphore_wait(barrier, 5)

    sent = []

    def send(src, dst, send_sem, recv_sem, peer):
        copy = pltpu.make_async_remote_copy(
            src_ref=src,
            dst_ref=dst,
            send_sem=send_sem,
            recv_sem=recv_sem,
            device_id=peer,
            device_id_type=pl.DeviceIdType.MESH,
        )
        copy.start()
        sent.append(copy)
        return copy

    def rows(c):
        return slice(c * ROWS, (c + 1) * ROWS)

    def cols_of(owner):
        return pl.ds(pl.multiple_of(owner * feat, feat), feat)

    def share(c):
        dst = full.at[rows(c), cols_of(me)]
        src = hidden.at[rows(c), :]
        a = send(src, dst, ag_send.at[0, c], ag_recv.at[0, c], {"tp": right})
        b = send(src, dst, ag_send.at[1, c], ag_recv.at[1, c], {"tp": left})
        return a, b

    def relay(c, pair):
        pair[0].wait_recv()
        pair[1].wait_recv()
        owner, peer = (left, right) if c % 2 == 0 else (right, left)
        block = full.at[rows(c), cols_of(owner)]
        return send(block, block, ag_send.at[2, c], ag_recv.at[2, c], {"tp": peer})

    half = model // 2

    def rel_block(b):
        for k in range(2):
            at = pl.ds(2 * b + k, 1)
            c_sin, c_cos = coarse[at, :half], coarse[at, half:]
            f_sin, f_cos = fine[:, :half], fine[:, half:]
            emb[rows(k), :half] = (c_sin * f_cos + c_cos * f_sin).astype(BF16)
            emb[rows(k), half:] = (c_cos * f_cos - c_sin * f_sin).astype(BF16)
        block = jnp.dot(emb[...], w_pos[...], preferred_element_type=F32)
        at = pl.ds(pl.multiple_of(b * 2 * ROWS, 2 * ROWS), 2 * ROWS)
        rel_t[:, at] = block.T.astype(BF16)

    blocks = span // (2 * ROWS)
    rel_cuts = [blocks * i // 3 for i in range(4)]

    def rel_some(i):
        def one(b, carry):
            rel_block(b)
            return carry

        lax.fori_loop(rel_cuts[i], rel_cuts[i + 1], one, 0)

    def project(c):
        x = full[rows(c), :]
        q = jnp.dot(x, w_all[:, :width], preferred_element_type=F32).astype(BF16).astype(F32)
        k = jnp.dot(x, w_all[:, width : 2 * width], preferred_element_type=F32)
        v = jnp.dot(x, w_all[:, 2 * width :], preferred_element_type=F32)
        lo = memory + c * ROWS
        k_t[:, lo : lo + ROWS] = k.T.astype(BF16)
        val[lo : lo + ROWS, :] = v.astype(BF16)
        for h in range(heads):
            at = slice(h * head_dim, (h + 1) * head_dim)
            cq[rows(c), at] = (q[:, at] + bias_c[h : h + 1, :]).astype(BF16)
            pq[rows(c), at] = (q[:, at] + bias_p[h : h + 1, :]).astype(BF16)

    def pass_on(hop, c):
        lo = (2 - hop) * seg + c * ROWS
        to = lo - seg
        peer = {"seq": following}
        a = send(
            k_t.at[:, lo : lo + ROWS],
            k_t.at[:, to : to + ROWS],
            kv_send.at[hop, 0, c],
            kv_recv.at[hop, 0, c],
            peer,
        )
        b = send(
            val.at[lo : lo + ROWS, :],
            val.at[to : to + ROWS, :],
            kv_send.at[hop, 1, c],
            kv_recv.at[hop, 1, c],
            peer,
        )
        return a, b

    pairs = [share(c) for c in range(2)]
    full[:, cols_of(me)] = hidden[...]
    loads[0].wait()
    loads[1].wait()
    relays, hops = [], [[], []]
    for c in range(chunks):
        if c < 3:
            rel_some(c)
        relays.append(relay(c, pairs[c]))
        if c + 2 < chunks:
            pairs.append(share(c + 2))
        if c == 1:
            for load in loads[2:5]:
                load.wait()
        if c >= 1:
            relays[c - 1].wait_recv()
            project(c - 1)
            hops[0].append(pass_on(0, c - 1))
    relays[-1].wait_recv()
    project(chunks - 1)
    hops[0].append(pass_on(0, chunks - 1))
    for c in range(chunks):
        for copy in hops[0][c]:
            copy.wait_recv()
        hops[1].append(pass_on(1, c))
    loads[5].wait()
    for c in range(chunks):
        for copy in hops[1][c]:
            copy.wait_recv()

    factor = np.float32(np.log2(np.e) / np.sqrt(head_dim))
    edge = jnp.maximum(memory - place * seg, 0)

    def attend(r, h, low):
        length = memory + (r + 1) * ROWS
        at = pl.ds(pl.multiple_of(h * head_dim, head_dim), head_dim)
        content = jnp.dot(cq[rows(r), at], k_t[at, :length], preferred_element_type=F32)
        position = jnp.dot(pq[rows(r), at], rel_t[at, span - length :], preferred_element_type=F32)
        position = pltpu.roll(position, length - (ROWS - 1), 1, stride=1, stride_axis=0)
        score = content + position + low
        last = score[:, length - ROWS :]
        i = lax.broadcasted_iota(jnp.int32, (ROWS, ROWS), 0)
        j = lax.broadcasted_iota(jnp.int32, (ROWS, ROWS), 1)
        last = jnp.where(j <= i, last, -1e30)
        score = jnp.concatenate([score[:, : length - ROWS], last], 1)
        top = jnp.max(score, axis=1, keepdims=True)
        e = jnp.exp2((score - top) * factor)
        probs = (e * (1.0 / jnp.sum(e, axis=1, keepdims=True))).astype(BF16)
        res = jnp.dot(probs, val[:length, at], preferred_element_type=F32)
        att[:, at] = res.astype(BF16)

    def product(owner):
        return jnp.dot(att[...], w_out[:, cols_of(owner)], preferred_element_type=F32).astype(BF16)

    scatter = [[None] * chunks for _ in range(3)]

    def ways(r):
        return (right, left) if r % 2 == 0 else (left, right)

    def scatter_first(r):
        ahead, back = ways(r)
        part[0, rows(r), :] = product(opp)
        scatter[0][r] = send(
            part.at[0, rows(r), :],
            got.at[0, rows(r), :],
            rs_send.at[0, r],
            rs_recv.at[0, r],
            {"tp": ahead},
        )
        part[1, rows(r), :] = product(back)
        scatter[1][r] = send(
            part.at[1, rows(r), :],
            got.at[1, rows(r), :],
            rs_send.at[1, r],
            rs_recv.at[1, r],
            {"tp": back},
        )
        part[2, rows(r), :] = product(ahead)
        sum_own[rows(r), :] = hidden[rows(r), :].astype(F32) + product(me).astype(F32)

    def scatter_second(r):
        ahead, _ = ways(r)
        scatter[0][r].wait_recv()
        both = part[2, rows(r), :].astype(F32) + got[0, rows(r), :].astype(F32)
        part[2, rows(r), :] = both.astype(BF16)
        scatter[2][r] = send(
            part.at[2, rows(r), :],
            got.at[2, rows(r), :],
            rs_send.at[2, r],
            rs_recv.at[2, r],
            {"tp": ahead},
        )

    stats = [None] * chunks

    def moments(r):
        scatter[1][r].wait_recv()
        scatter[2][r].wait_recv()
        y = sum_own[rows(r), :] + got[1, rows(r), :].astype(F32) + got[2, rows(r), :].astype(F32)
        sum_own[rows(r), :] = y
        total = jnp.sum(y, axis=1, keepdims=True)
        off = y - total * (1.0 / feat)
        square = jnp.sum(off * off, axis=1, keepdims=True)
        lane = lax.broadcasted_iota(jnp.int32, (ROWS, ROWS), 1)
        tile = jnp.where(lane == 0, total, square)
        stat[r] = tile.T[:8, :]
        stats[r] = [
            send(stat.at[r], stat_got.at[i, r], st_send.at[i, r], st_recv.at[i, r], {"tp": peer})
            for i, peer in enumerate((right, left, opp))
        ]

    def finish(r):
        for copy in stats[r]:
            copy.wait_recv()
        all_of = [stat[r]] + [stat_got[i, r] for i in range(3)]
        totals = [a[0:1, :] for a in all_of]
        squares = [a[1:2, :] for a in all_of]
        center = sum(totals[1:], totals[0]) * (1.0 / model)
        spread = sum(squares[1:], squares[0])
        for t in totals:
            gap = t * (1.0 / feat) - center
            spread = spread + feat * (gap * gap)
        inverse = 1.0 / jnp.sqrt(spread * (1.0 / model) + 1e-05)
        center = jnp.broadcast_to(center, (ROWS, ROWS)).T
        inverse = jnp.broadcast_to(inverse, (ROWS, ROWS)).T
        for p in range(feat // ROWS):
            at = slice(p * ROWS, (p + 1) * ROWS)
            y = (sum_own[rows(r), at] - center) * inverse
            out[rows(r), at] = (y * gain[:, at] + shift[:, at]).astype(BF16)

    for r in range(chunks):
        length = memory + (r + 1) * ROWS
        col = lax.broadcasted_iota(jnp.int32, (1, length), 1)
        low = jnp.where(col >= edge, 0.0, -1e30).astype(F32)

        def two(p, carry):
            attend(r, 2 * p, low)
            attend(r, 2 * p + 1, low)
            return carry

        lax.fori_loop(0, heads // 2, two, 0)
        scatter_first(r)
        if r >= 1:
            scatter_second(r - 1)
        if r >= 2:
            moments(r - 2)
    scatter_second(chunks - 1)
    moments(chunks - 2)
    moments(chunks - 1)
    for r in range(chunks):
        finish(r)
    for copy in sent:
        copy.wait_send()


def shards(n_seq, n_tp, hidden_in, wq, wk, wv, w_pos, w_out, bias_c, bias_p, gain, shift):
    seg, feat = hidden_in.shape
    heads, head_dim = bias_c.shape
    model, width = wq.shape
    span = 3 * seg
    chunks = seg // ROWS
    fine, coarse = angle_tables(span, model)
    any_spec = pl.BlockSpec(memory_space=pl.ANY)
    vmem = pl.BlockSpec(memory_space=pltpu.VMEM)
    dma = pltpu.SemaphoreType.DMA
    return pl.pallas_call(
        functools.partial(kernel, n_seq, n_tp),
        out_shape=jax.ShapeDtypeStruct((seg, feat), BF16),
        in_specs=[vmem] + [any_spec] * 6 + [vmem] * 5,
        out_specs=vmem,
        scratch_shapes=[
            pltpu.VMEM((model, 3 * width), BF16),
            pltpu.VMEM((model, width), BF16),
            pltpu.VMEM((width, model), BF16),
            pltpu.VMEM((ROWS, model), F32),
            pltpu.VMEM((seg, model), BF16),
            pltpu.VMEM((width, span), BF16),
            pltpu.VMEM((span, width), BF16),
            pltpu.VMEM((width, span), BF16),
            pltpu.VMEM((2 * ROWS, model), BF16),
            pltpu.VMEM((seg, width), BF16),
            pltpu.VMEM((seg, width), BF16),
            pltpu.VMEM((ROWS, width), BF16),
            pltpu.VMEM((seg, feat), F32),
            pltpu.VMEM((3, seg, feat), BF16),
            pltpu.VMEM((3, seg, feat), BF16),
            pltpu.VMEM((chunks, 8, ROWS), F32),
            pltpu.VMEM((3, chunks, 8, ROWS), F32),
            dma((6,)),
            dma((3, chunks)),
            dma((3, chunks)),
            dma((2, 2, chunks)),
            dma((2, 2, chunks)),
            dma((3, chunks)),
            dma((3, chunks)),
            dma((3, chunks)),
            dma((3, chunks)),
        ],
        compiler_params=pltpu.CompilerParams(
            collective_id=0, has_side_effects=True, vmem_limit_bytes=60 * 1024 * 1024
        ),
        name="layer",
    )(
        hidden_in,
        wq,
        wk,
        wv,
        w_pos,
        w_out,
        jnp.asarray(fine),
        jnp.asarray(coarse),
        bias_c,
        bias_p,
        gain.reshape(1, feat),
        shift.reshape(1, feat),
    )


def solution(mesh):
    in_specs = (
        P("seq", "tp"),
        P(None, "tp"),
        P(None, "tp"),
        P(None, "tp"),
        P(None, "tp"),
        P("tp", None),
        P("tp", None),
        P("tp", None),
        P("tp"),
        P("tp"),
    )
    return jax.shard_map(
        functools.partial(shards, mesh.shape["seq"], mesh.shape["tp"]),
        mesh=mesh,
        in_specs=in_specs,
        out_specs=P("seq", "tp"),
        check_vma=False,
    )
```

```python
import functools

import jax
import jax.numpy as jnp
import numpy as np
from jax import lax
from jax.experimental import pallas as pl
from jax.experimental.pallas import tpu as pltpu
from jax.sharding import PartitionSpec as P

F32 = jnp.float32
BF16 = jnp.bfloat16
ROWS = 128


def angle_tables(span, width):
    half = width // 2
    freq = np.exp(-np.log(10000.0) * np.arange(half) / half)
    fine = (ROWS - 1 - np.arange(ROWS))[:, None] * freq[None]
    blocks = span // ROWS
    coarse = (ROWS * (blocks - 1 - np.arange(blocks)))[:, None] * freq[None]
    pack = lambda a: np.concatenate([np.sin(a), np.cos(a)], 1).astype(np.float32)
    return pack(fine), pack(coarse)


def kernel(
    n_seq,
    n_tp,
    hidden,
    wq_hbm,
    wk_hbm,
    wv_hbm,
    wpos_hbm,
    wout_hbm,
    fine_hbm,
    coarse,
    bias_c,
    bias_p,
    gain,
    shift,
    out,
    w_all,
    w_pos,
    w_out,
    fine,
    full,
    k_t,
    val,
    rel_t,
    emb,
    cq,
    pq,
    att,
    sum_own,
    part,
    got,
    stat,
    stat_got,
    local_sem,
    ag_send,
    ag_recv,
    kv_send,
    kv_recv,
    rs_send,
    rs_recv,
    st_send,
    st_recv,
):
    seg, feat = hidden.shape
    heads, head_dim = bias_c.shape
    width = heads * head_dim
    model = n_tp * feat
    span = 3 * seg
    memory = 2 * seg
    chunks = seg // ROWS
    me = lax.axis_index("tp")
    place = lax.axis_index("seq")
    right = lax.rem(me + 1, n_tp)
    left = lax.rem(me + n_tp - 1, n_tp)
    opp = lax.rem(me + 2, n_tp)
    following = lax.rem(place + 1, n_seq)
    before = lax.rem(place + n_seq - 1, n_seq)

    loads = []
    for i, (src, dst) in enumerate(
        (
            (fine_hbm, fine),
            (wpos_hbm, w_pos),
            (wq_hbm, w_all.at[:, 0:width]),
            (wk_hbm, w_all.at[:, width : 2 * width]),
            (wv_hbm, w_all.at[:, 2 * width : 3 * width]),
            (wout_hbm, w_out),
        )
    ):
        load = pltpu.make_async_copy(src, dst, local_sem.at[i])
        load.start()
        loads.append(load)

    barrier = pltpu.get_barrier_semaphore()
    for peer in ({"tp": right}, {"tp": left}, {"tp": opp}, {"seq": following}, {"seq": before}):
        pl.semaphore_signal(barrier, inc=1, device_id=peer, device_id_type=pl.DeviceIdType.MESH)
    pl.semaphore_wait(barrier, 5)

    sent = []

    def send(src, dst, send_sem, recv_sem, peer):
        copy = pltpu.make_async_remote_copy(
            src_ref=src,
            dst_ref=dst,
            send_sem=send_sem,
            recv_sem=recv_sem,
            device_id=peer,
            device_id_type=pl.DeviceIdType.MESH,
        )
        copy.start()
        sent.append(copy)
        return copy

    def rows(c):
        return slice(c * ROWS, (c + 1) * ROWS)

    def cols_of(owner):
        return pl.ds(pl.multiple_of(owner * feat, feat), feat)

    step = ROWS // 2

    def piece(c):
        return slice(c * step, (c + 1) * step)

    def share(way, c):
        peer = left if way else right
        return send(
            hidden.at[piece(c), :],
            full.at[piece(c), cols_of(me)],
            ag_send.at[way, c],
            ag_recv.at[way, c],
            {"tp": peer},
        )

    def relay(way, c):
        owner, peer = (right, left) if way else (left, right)
        block = full.at[piece(c), cols_of(owner)]
        return send(block, block, ag_send.at[2, c], ag_recv.at[2, c], {"tp": peer})

    half = model // 2

    def rel_block(b):
        for k in range(2):
            at = pl.ds(2 * b + k, 1)
            c_sin, c_cos = coarse[at, :half], coarse[at, half:]
            f_sin, f_cos = fine[:, :half], fine[:, half:]
            emb[rows(k), :half] = (c_sin * f_cos + c_cos * f_sin).astype(BF16)
            emb[rows(k), half:] = (c_cos * f_cos - c_sin * f_sin).astype(BF16)
        block = jnp.dot(emb[...], w_pos[...], preferred_element_type=F32)
        at = pl.ds(pl.multiple_of(b * 2 * ROWS, 2 * ROWS), 2 * ROWS)
        rel_t[:, at] = block.T.astype(BF16)

    blocks = span // (2 * ROWS)
    rel_cuts = [blocks * i // chunks for i in range(chunks + 1)]

    def rel_some(i):
        def one(b, carry):
            rel_block(b)
            return carry

        lax.fori_loop(rel_cuts[i], rel_cuts[i + 1], one, 0)

    def project(c):
        x = full[rows(c), :]
        q = jnp.dot(x, w_all[:, :width], preferred_element_type=F32).astype(BF16).astype(F32)
        k = jnp.dot(x, w_all[:, width : 2 * width], preferred_element_type=F32)
        v = jnp.dot(x, w_all[:, 2 * width :], preferred_element_type=F32)
        lo = memory + c * ROWS
        k_t[:, lo : lo + ROWS] = k.T.astype(BF16)
        val[lo : lo + ROWS, :] = v.astype(BF16)
        for h in range(heads):
            at = slice(h * head_dim, (h + 1) * head_dim)
            cq[rows(c), at] = (q[:, at] + bias_c[h : h + 1, :]).astype(BF16)
            pq[rows(c), at] = (q[:, at] + bias_p[h : h + 1, :]).astype(BF16)

    def pass_on(hop, c):
        lo = (2 - hop) * seg + c * ROWS
        to = lo - seg
        peer = {"seq": following}
        a = send(
            k_t.at[:, lo : lo + ROWS],
            k_t.at[:, to : to + ROWS],
            kv_send.at[hop, 0, c],
            kv_recv.at[hop, 0, c],
            peer,
        )
        b = send(
            val.at[lo : lo + ROWS, :],
            val.at[to : to + ROWS, :],
            kv_send.at[hop, 1, c],
            kv_recv.at[hop, 1, c],
            peer,
        )
        return a, b

    order = [[c + way if c % 2 == 0 else c - way for c in range(2 * chunks)] for way in range(2)]
    shared, relays, hops = {}, {}, [[], []]

    def share_next(first, last):
        for at in range(first, min(last, 2 * chunks)):
            for way in range(2):
                shared[way, order[way][at]] = share(way, order[way][at])

    def gathered(p):
        shared[0, 2 * p + 1].wait_recv()
        shared[1, 2 * p].wait_recv()
        relays[2 * p].wait_recv()
        relays[2 * p + 1].wait_recv()
        project(p)
        hops[0].append(pass_on(0, p))

    def forward(p):
        for copy in hops[0][p]:
            copy.wait_recv()
        hops[1].append(pass_on(1, p))

    share_next(0, 3)
    full[:, cols_of(me)] = hidden[...]
    loads[0].wait()
    loads[1].wait()
    for p in range(chunks):
        for way in range(2):
            shared[way, 2 * p + way].wait_recv()
            relays[2 * p + way] = relay(way, 2 * p + way)
        share_next(2 * p + 3, 2 * p + 5)
        if p == 1:
            for load in loads[2:5]:
                load.wait()
        if p >= 1:
            gathered(p - 1)
        if p >= 2:
            forward(p - 2)
        rel_some(p)
    gathered(chunks - 1)
    forward(chunks - 2)
    forward(chunks - 1)
    loads[5].wait()
    for c in range(chunks):
        for copy in hops[1][c]:
            copy.wait_recv()

    factor = np.float32(np.log2(np.e) / np.sqrt(head_dim))
    edge = jnp.maximum(memory - place * seg, 0)

    def attend(r, h, low):
        length = memory + (r + 1) * ROWS
        at = pl.ds(pl.multiple_of(h * head_dim, head_dim), head_dim)
        content = jnp.dot(cq[rows(r), at], k_t[at, :length], preferred_element_type=F32)
        position = jnp.dot(pq[rows(r), at], rel_t[at, span - length :], preferred_element_type=F32)
        position = pltpu.roll(position, length - (ROWS - 1), 1, stride=1, stride_axis=0)
        score = content + position + low
        last = score[:, length - ROWS :]
        i = lax.broadcasted_iota(jnp.int32, (ROWS, ROWS), 0)
        j = lax.broadcasted_iota(jnp.int32, (ROWS, ROWS), 1)
        last = jnp.where(j <= i, last, -1e30)
        score = jnp.concatenate([score[:, : length - ROWS], last], 1)
        top = jnp.max(score, axis=1, keepdims=True)
        e = jnp.exp2((score - top) * factor)
        probs = (e * (1.0 / jnp.sum(e, axis=1, keepdims=True))).astype(BF16)
        res = jnp.dot(probs, val[:length, at], preferred_element_type=F32)
        att[:, at] = res.astype(BF16)

    def product(owner):
        return jnp.dot(att[...], w_out[:, cols_of(owner)], preferred_element_type=F32).astype(BF16)

    scatter = [[None] * chunks for _ in range(3)]

    def ways(r):
        return (right, left) if r % 2 == 0 else (left, right)

    def scatter_first(r):
        ahead, back = ways(r)
        part[0, rows(r), :] = product(opp)
        scatter[0][r] = send(
            part.at[0, rows(r), :],
            got.at[0, rows(r), :],
            rs_send.at[0, r],
            rs_recv.at[0, r],
            {"tp": ahead},
        )
        part[1, rows(r), :] = product(back)
        scatter[1][r] = send(
            part.at[1, rows(r), :],
            got.at[1, rows(r), :],
            rs_send.at[1, r],
            rs_recv.at[1, r],
            {"tp": back},
        )
        part[2, rows(r), :] = product(ahead)
        sum_own[rows(r), :] = hidden[rows(r), :].astype(F32) + product(me).astype(F32)

    def scatter_second(r):
        ahead, _ = ways(r)
        scatter[0][r].wait_recv()
        both = part[2, rows(r), :].astype(F32) + got[0, rows(r), :].astype(F32)
        part[2, rows(r), :] = both.astype(BF16)
        scatter[2][r] = send(
            part.at[2, rows(r), :],
            got.at[2, rows(r), :],
            rs_send.at[2, r],
            rs_recv.at[2, r],
            {"tp": ahead},
        )

    stats = [None] * chunks

    def moments(r):
        scatter[1][r].wait_recv()
        scatter[2][r].wait_recv()
        y = sum_own[rows(r), :] + got[1, rows(r), :].astype(F32) + got[2, rows(r), :].astype(F32)
        sum_own[rows(r), :] = y
        total = jnp.sum(y, axis=1, keepdims=True)
        off = y - total * (1.0 / feat)
        square = jnp.sum(off * off, axis=1, keepdims=True)
        lane = lax.broadcasted_iota(jnp.int32, (ROWS, ROWS), 1)
        tile = jnp.where(lane == 0, total, square)
        stat[r] = tile.T[:8, :]
        stats[r] = [
            send(stat.at[r], stat_got.at[i, r], st_send.at[i, r], st_recv.at[i, r], {"tp": peer})
            for i, peer in enumerate((right, left, opp))
        ]

    def finish(r):
        for copy in stats[r]:
            copy.wait_recv()
        all_of = [stat[r]] + [stat_got[i, r] for i in range(3)]
        totals = [a[0:1, :] for a in all_of]
        squares = [a[1:2, :] for a in all_of]
        center = sum(totals[1:], totals[0]) * (1.0 / model)
        spread = sum(squares[1:], squares[0])
        for t in totals:
            gap = t * (1.0 / feat) - center
            spread = spread + feat * (gap * gap)
        inverse = 1.0 / jnp.sqrt(spread * (1.0 / model) + 1e-05)
        center = jnp.broadcast_to(center, (ROWS, ROWS)).T
        inverse = jnp.broadcast_to(inverse, (ROWS, ROWS)).T
        for p in range(feat // ROWS):
            at = slice(p * ROWS, (p + 1) * ROWS)
            y = (sum_own[rows(r), at] - center) * inverse
            out[rows(r), at] = (y * gain[:, at] + shift[:, at]).astype(BF16)

    for r in range(chunks):
        length = memory + (r + 1) * ROWS
        col = lax.broadcasted_iota(jnp.int32, (1, length), 1)
        low = jnp.where(col >= edge, 0.0, -1e30).astype(F32)

        def two(p, carry):
            attend(r, 2 * p, low)
            attend(r, 2 * p + 1, low)
            return carry

        lax.fori_loop(0, heads // 2, two, 0)
        scatter_first(r)
        if r >= 1:
            scatter_second(r - 1)
        if r >= 2:
            moments(r - 2)
    scatter_second(chunks - 1)
    moments(chunks - 2)
    moments(chunks - 1)
    for r in range(chunks):
        finish(r)
    for copy in sent:
        copy.wait_send()


def shards(n_seq, n_tp, hidden_in, wq, wk, wv, w_pos, w_out, bias_c, bias_p, gain, shift):
    seg, feat = hidden_in.shape
    heads, head_dim = bias_c.shape
    model, width = wq.shape
    span = 3 * seg
    chunks = seg // ROWS
    fine, coarse = angle_tables(span, model)
    any_spec = pl.BlockSpec(memory_space=pl.ANY)
    vmem = pl.BlockSpec(memory_space=pltpu.VMEM)
    dma = pltpu.SemaphoreType.DMA
    return pl.pallas_call(
        functools.partial(kernel, n_seq, n_tp),
        out_shape=jax.ShapeDtypeStruct((seg, feat), BF16),
        in_specs=[vmem] + [any_spec] * 6 + [vmem] * 5,
        out_specs=vmem,
        scratch_shapes=[
            pltpu.VMEM((model, 3 * width), BF16),
            pltpu.VMEM((model, width), BF16),
            pltpu.VMEM((width, model), BF16),
            pltpu.VMEM((ROWS, model), F32),
            pltpu.VMEM((seg, model), BF16),
            pltpu.VMEM((width, span), BF16),
            pltpu.VMEM((span, width), BF16),
            pltpu.VMEM((width, span), BF16),
            pltpu.VMEM((2 * ROWS, model), BF16),
            pltpu.VMEM((seg, width), BF16),
            pltpu.VMEM((seg, width), BF16),
            pltpu.VMEM((ROWS, width), BF16),
            pltpu.VMEM((seg, feat), F32),
            pltpu.VMEM((3, seg, feat), BF16),
            pltpu.VMEM((3, seg, feat), BF16),
            pltpu.VMEM((chunks, 8, ROWS), F32),
            pltpu.VMEM((3, chunks, 8, ROWS), F32),
            dma((6,)),
            dma((3, 2 * chunks)),
            dma((3, 2 * chunks)),
            dma((2, 2, chunks)),
            dma((2, 2, chunks)),
            dma((3, chunks)),
            dma((3, chunks)),
            dma((3, chunks)),
            dma((3, chunks)),
        ],
        compiler_params=pltpu.CompilerParams(
            collective_id=0, has_side_effects=True, vmem_limit_bytes=60 * 1024 * 1024
        ),
        name="layer",
    )(
        hidden_in,
        wq,
        wk,
        wv,
        w_pos,
        w_out,
        jnp.asarray(fine),
        jnp.asarray(coarse),
        bias_c,
        bias_p,
        gain.reshape(1, feat),
        shift.reshape(1, feat),
    )


def solution(mesh):
    in_specs = (
        P("seq", "tp"),
        P(None, "tp"),
        P(None, "tp"),
        P(None, "tp"),
        P(None, "tp"),
        P("tp", None),
        P("tp", None),
        P("tp", None),
        P("tp"),
        P("tp"),
    )
    return jax.shard_map(
        functools.partial(shards, mesh.shape["seq"], mesh.shape["tp"]),
        mesh=mesh,
        in_specs=in_specs,
        out_specs=P("seq", "tp"),
        check_vma=False,
    )
```
